32 devices in a mesh: space: 4 (over y, x), dp: 8 (over z, core).
Axes of the slice: x: 2, y: 2, z: 4, core: 2. Of those that a mesh axis runs over, the one named last changes fastest.
Arguments:
- mixed_two: bfloat16 [8, 16, 180, 768], P('dp', 'space'), may hold values from -6 to 6
- input_two: bfloat16 [8, 16, 180, 768], P('dp', 'space'), may hold values from -6 to 6
- cotangent: bfloat16 [8, 16, 180, 768], P('dp', 'space'), may hold values from -6 to 6
- w_in_two: bfloat16 [3072, 768], replicated, may hold values from -0.21875 to 0.21875
- w_out_two: bfloat16 [3072, 768], replicated, may hold values from -0.109375 to 0.109375
- kernel_two: bfloat16 [9, 768], replicated, may hold values from -2 to 2
- mixed_one: bfloat16 [8, 16, 180, 768], P('dp', 'space'), may hold values from -6 to 6
- w_in_one: bfloat16 [3072, 768], replicated, may hold values from -0.21875 to 0.21875
- w_out_one: bfloat16 [3072, 768], replicated, may hold values from -0.109375 to 0.109375
- kernel_one: bfloat16 [9, 768], replicated, may hold values from -2 to 2
Outputs:
- input_grad: bfloat16 [8, 16, 180, 768], P('dp', 'space')
- grad_w_in: float32 [3072, 768], P('dp')
- grad_w_out: float32 [3072, 768], P('dp')
- grad_kernel: float32 [9, 768], replicated
The draws below stay inside these ranges and needn't reach their ends.
All inputs are finite; a program needn't handle non-finite values.
Results may differ from the reference program's by a relative error of at most 0.02.
Values may be sent and summed in bfloat16 or wider, within the bound.
A program may use at most 192 MiB of HBM per device.

```python
import math
import jax
import jax.numpy as jnp
from jax import lax

D = 768
FF = 3072
LON = 180
LAT = 16
BATCH = 8
TAPS = 9


def shard_levels(stream_key, extent, cuts, smallest, top_value):
    loudness = 1.0
    for dim, parts in cuts:
        steps = jax.random.uniform(jax.random.fold_in(jax.random.fold_in(stream_key, 6), dim), (parts,), jnp.float32, smallest / len(cuts), top_value / len(cuts))
        loudness = loudness * jnp.repeat(jnp.exp(steps), extent[dim] // parts).reshape((-1,) + (1,) * (len(extent) - 1 - dim))
    return loudness


def bell_draw(key, dims, width, limit, shards=(), held_as=jnp.bfloat16):
    drawn = jax.random.normal(key, dims, jnp.float32) * width
    if len(shards) > 0:
        drawn = shard_levels(key, dims, shards, -0.22, 0.18) * drawn
    return jnp.clip(drawn, min=-limit, max=limit).astype(held_as)


def setup_inputs(seed: int = 0) -> dict:
    seeds = jax.random.split(jax.random.key(seed), 11)
    mixed_two = bell_draw(seeds[0], (BATCH, LAT, LON, D), 1.0, 6.0, ((0, 8), (1, 4)))
    input_two = bell_draw(seeds[1], (BATCH, LAT, LON, D), 1.0, 6.0, ((0, 8), (1, 4)))
    cotangent = bell_draw(seeds[2], (BATCH, LAT, LON, D), 1.0, 6.0, ((0, 8), (1, 4)))
    w_in_two = bell_draw(seeds[3], (FF, D), D ** -0.5, 0.21875)
    w_out_two = bell_draw(seeds[4], (FF, D), FF ** -0.5, 0.109375)
    kernel_two = bell_draw(seeds[5], (TAPS, D), 0.35, 2.0)
    mixed_one = bell_draw(seeds[6], (BATCH, LAT, LON, D), 1.0, 6.0, ((0, 8), (1, 4)))
    w_in_one = bell_draw(seeds[7], (FF, D), D ** -0.5, 0.21875)
    w_out_one = bell_draw(seeds[8], (FF, D), FF ** -0.5, 0.109375)
    kernel_one = bell_draw(seeds[9], (TAPS, D), 0.35, 2.0)
    return {"mixed_two": mixed_two, "input_two": input_two, "cotangent": cotangent, "w_in_two": w_in_two, "w_out_two": w_out_two, "kernel_two": kernel_two, "mixed_one": mixed_one, "w_in_one": w_in_one, "w_out_one": w_out_one, "kernel_one": kernel_one}


GELU_C = math.sqrt(2.0 / math.pi)
CONTRACT_LAST = (((1,), (1,)), ((), ()))
CONTRACT_FIRST = (((0,), (0,)), ((), ()))

def gelu_parts(preact):
    tanh_arg = GELU_C * (preact + 0.044715 * preact * preact * preact)
    tanh_val = jnp.tanh(tanh_arg)
    activation = 0.5 * preact * (1.0 + tanh_val)
    gelu_slope = 0.5 * (1.0 + tanh_val) + 0.5 * preact * (1.0 - tanh_val * tanh_val) * GELU_C * (1.0 + 3.0 * 0.044715 * preact * preact)
    return (activation, gelu_slope)

def pad_rows(field):
    return jnp.pad(field, ((0, 0), (1, 1), (0, 0), (0, 0)))

def conv_back(padded, kernel, band_rows):
    kernel_f = kernel.astype(jnp.float32)
    result = jnp.zeros(padded[:, 1:1 + band_rows].shape, jnp.float32)
    for lat_off in range(3):
        for lon_off in range(3):
            window = padded[:, 2 - lat_off:2 - lat_off + band_rows].astype(jnp.float32)
            result = result + kernel_f[3 * lat_off + lon_off] * jnp.roll(window, lon_off - 1, axis=2)
    return result

def kernel_terms(padded_in, mix_grad, band_rows):
    grad_f = mix_grad.astype(jnp.float32)
    collected = []
    for lat_off in range(3):
        for lon_off in range(3):
            window = jnp.roll(padded_in[:, lat_off:lat_off + band_rows], 1 - lon_off, axis=2)
            collected.append(lax.optimization_barrier(jnp.sum(window.astype(jnp.float32) * grad_f, axis=(0, 1, 2))))
    return jnp.stack(collected)

def reference(mixed_two, input_two, cotangent, w_in_two, w_out_two, kernel_two, mixed_one, w_in_one, w_out_one, kernel_one):

    def sample_pass(items):
        mixed_late, input_late, cot_late, mixed_early = [item[None] for item in items]
        shape4 = mixed_late.shape
        band_rows = shape4[1]
        channels = shape4[3]
        mixed_flat = mixed_late.reshape(-1, channels)
        cot_flat = cot_late.reshape(-1, channels)
        preact = lax.dot_general(mixed_flat, w_in_two, CONTRACT_LAST, preferred_element_type=jnp.float32)
        activation, gelu_slope = gelu_parts(preact)
        activation = activation.astype(jnp.bfloat16)
        hidden_grad = lax.dot_general(cot_flat, w_out_two, CONTRACT_LAST, preferred_element_type=jnp.float32)
        pre_grad = (hidden_grad * gelu_slope).astype(jnp.bfloat16)
        mix_grad = jnp.dot(pre_grad, w_in_two, preferred_element_type=jnp.float32).astype(jnp.bfloat16).reshape(shape4)
        out_term = lax.dot_general(activation, cot_flat, CONTRACT_FIRST, preferred_element_type=jnp.float32)
        in_term = lax.dot_general(pre_grad, mixed_flat, CONTRACT_FIRST, preferred_element_type=jnp.float32)
        taps_term = kernel_terms(pad_rows(input_late), mix_grad, band_rows)
        grad_two = (cot_late.astype(jnp.float32) + conv_back(pad_rows(mix_grad), kernel_two, band_rows)).astype(jnp.bfloat16)
        preact_early = lax.dot_general(mixed_early.reshape(-1, channels), w_in_one, CONTRACT_LAST, preferred_element_type=jnp.float32)
        unused_act, slope_early = gelu_parts(preact_early)
        hidden_early = lax.dot_general(grad_two.reshape(-1, channels), w_out_one, CONTRACT_LAST, preferred_element_type=jnp.float32)
        pre_early = (hidden_early * slope_early).astype(jnp.bfloat16)
        mix_early = jnp.dot(pre_early, w_in_one, preferred_element_type=jnp.float32).astype(jnp.bfloat16).reshape(shape4)
        grad_one = (grad_two.astype(jnp.float32) + conv_back(pad_rows(mix_early), kernel_one, band_rows)).astype(jnp.bfloat16)
        return (grad_one[0], in_term, out_term, taps_term)
    grad_one, in_terms, out_terms, tap_terms = lax.map(sample_pass, (mixed_two, input_two, cotangent, mixed_one))
    grad_w_in = lax.optimization_barrier(jnp.sum(in_terms, axis=0)) / BATCH
    grad_w_out = lax.optimization_barrier(jnp.sum(out_terms, axis=0)) / BATCH
    grad_kernel = lax.optimization_barrier(jnp.sum(tap_terms, axis=0)) / BATCH
    return (grad_one, grad_w_in, grad_w_out, grad_kernel)
```

```python
import math

import jax
import jax.numpy as jnp
from jax import lax
from jax.experimental import pallas as pl
from jax.experimental.pallas import tpu as pltpu
from jax.sharding import PartitionSpec as P

GELU_C = math.sqrt(2.0 / math.pi)
CONTRACT_LAST = (((1,), (1,)), ((), ()))
CONTRACT_FIRST = (((0,), (0,)), ((), ()))


LANES = 128


def edge_rows(cells):
    count = lax.axis_size("space")
    ends = count - 1
    head = cells[:, :1]
    tail = cells[:, -1:]
    before = lax.ppermute(tail, "space", [(i, i + 1) for i in range(ends)])
    after = lax.ppermute(head, "space", [(i + 1, i) for i in range(ends)])
    return before, after


def rolled(row, shift):
    if shift == 0:
        return row
    if shift == 1:
        return jnp.concatenate([row[-1:], row[:-1]], axis=0)
    return jnp.concatenate([row[1:], row[:1]], axis=0)


def spread(ref_before, ref, ref_after, index, band_rows):
    if index == 0:
        return ref_before[0, 0]
    if index == band_rows + 1:
        return ref_after[0, 0]
    return ref[0, index - 1]


def conv_accumulate(out_ref, base_ref, kernel_ref, before_ref, grad_ref, after_ref, visit):
    band_rows = grad_ref.shape[1]
    taps = kernel_ref[...].astype(jnp.float32)
    windows = {}
    for i in range(band_rows):
        for p in range(i, i + 3):
            if p not in windows:
                row = spread(before_ref, grad_ref, after_ref, p, band_rows).astype(jnp.float32)
                windows[p] = [rolled(row, b - 1) for b in range(3)]
        total = base_ref[0, i].astype(jnp.float32)
        for lat in range(3):
            for lon in range(3):
                tap = 3 * lat + lon
                total = total + taps[tap : tap + 1] * windows[i + 2 - lat][lon]
        out_ref[0, i] = total.astype(out_ref.dtype)
        visit(i, windows[i + 1])
        del windows[i]


def late_kernel(
    base_ref, kernel_ref, before_ref, grad_ref, after_ref,
    in_before_ref, in_ref, in_after_ref, out_ref, taps_ref,
):
    band_rows = grad_ref.shape[1]
    taps_ref[...] = jnp.zeros_like(taps_ref)

    def visit(i, shifted):
        for lat in range(3):
            row = spread(in_before_ref, in_ref, in_after_ref, i + lat, band_rows)
            row = row.astype(jnp.float32)
            for lon in range(3):
                tap = 3 * lat + lon
                taps_ref[tap : tap + 1, :] += jnp.sum(row * shifted[lon], axis=0, keepdims=True)

    conv_accumulate(out_ref, base_ref, kernel_ref, before_ref, grad_ref, after_ref, visit)


def early_kernel(base_ref, kernel_ref, before_ref, grad_ref, after_ref, out_ref):
    conv_accumulate(
        out_ref, base_ref, kernel_ref, before_ref, grad_ref, after_ref, lambda i, w: None
    )


def conv_call(kernel_fn, base, kernel, edges, grad, more, with_taps):
    samples, rows, columns, channels = grad.shape
    taps = kernel.shape[0]

    def field(count):
        return pl.BlockSpec((1, count, columns, LANES), lambda s, c: (s, 0, 0, c))

    tap_spec = pl.BlockSpec((taps, LANES), lambda s, c: (0, c))
    in_specs = [field(rows), tap_spec, field(1), field(rows), field(1)]
    args = [base, kernel, edges[0], grad, edges[1]]
    out_shape = [jax.ShapeDtypeStruct(grad.shape, jnp.bfloat16)]
    out_specs = [field(rows)]
    if with_taps:
        in_specs += [field(1), field(rows), field(1)]
        args += more
        out_shape.append(jax.ShapeDtypeStruct((samples, taps, channels), jnp.float32))
        out_specs.append(pl.BlockSpec((None, taps, LANES), lambda s, c: (s, 0, c)))
    work = grad.size * (40 if with_taps else 20)
    return pl.pallas_call(
        kernel_fn,
        grid=(samples, channels // LANES),
        in_specs=in_specs,
        out_specs=out_specs,
        out_shape=out_shape,
        compiler_params=pltpu.CompilerParams(
            dimension_semantics=("arbitrary", "arbitrary"), vmem_limit_bytes=24 * 1024 * 1024
        ),
        cost_estimate=pl.CostEstimate(
            flops=work, bytes_accessed=grad.size * 8, transcendentals=0
        ),
    )(*args)


def gelu_parts(preact):
    tanh_arg = GELU_C * (preact + 0.044715 * preact * preact * preact)
    tanh_val = jnp.tanh(tanh_arg)
    activation = 0.5 * preact * (1.0 + tanh_val)
    gelu_slope = 0.5 * (1.0 + tanh_val) + 0.5 * preact * (1.0 - tanh_val * tanh_val) * GELU_C * (
        1.0 + 3.0 * 0.044715 * preact * preact
    )
    return (activation, gelu_slope)


def bits_of(axis):
    return (lax.axis_size(axis) - 1).bit_length()


def swap(cells, axis, bit):
    count = lax.axis_size(axis)
    return lax.ppermute(cells, axis, [(i, i ^ (1 << bit)) for i in range(count)])


def my_bit(axis, bit):
    return (lax.axis_index(axis) // (1 << bit)) % 2


def split(cells, labels, axis, bit):
    dim = labels.index((axis, bit))
    mine = my_bit(axis, bit)
    sent = lax.dynamic_index_in_dim(cells, 1 - mine, dim, keepdims=False)
    kept = lax.dynamic_index_in_dim(cells, mine, dim, keepdims=False)
    return kept, swap(sent, axis, bit), labels[:dim] + labels[dim + 1 :]


def merged(kept, came):
    return (kept.astype(jnp.float32) + came.astype(jnp.float32)).astype(jnp.bfloat16)


def reduction(term):
    dp_bits, space_bits = bits_of("dp"), bits_of("space")
    labels = [("dp", bit) for bit in reversed(range(dp_bits))]
    labels += [("space", bit) for bit in reversed(range(space_bits))]
    width = term.shape[1]
    cells = term.reshape((2,) * len(labels) + (-1, width))
    kept, came, labels = split(cells, labels, "dp", 0)
    (came,) = yield [came]
    cells = merged(kept, came)
    halves = [
        lax.slice_in_dim(cells, part * width // 2, (part + 1) * width // 2, axis=cells.ndim - 1)
        for part in range(2)
    ]
    space_order = list(range(space_bits))
    rest = [("dp", bit) for bit in range(1, dp_bits)]
    orders = [
        [("space", bit) for bit in order] + rest for order in (space_order, space_order[::-1])
    ]
    left = [labels, labels]
    for step in range(len(orders[0])):
        moved = [split(halves[p], left[p], *orders[p][step]) for p in range(2)]
        left = [m[2] for m in moved]
        arrived = yield [m[1] for m in moved]
        halves = [merged(m[0], c) for m, c in zip(moved, arrived)]
    halves = [half[None] for half in halves]
    for bit in range(space_bits):
        others = yield [swap(half, "space", bit) for half in halves]
        low = my_bit("space", bit) == 0
        halves = [
            jnp.concatenate([jnp.where(low, h, o), jnp.where(low, o, h)], axis=0)
            for h, o in zip(halves, others)
        ]
    rows = jnp.concatenate([half.reshape(-1, width // 2) for half in halves], axis=1)
    return rows.astype(jnp.float32)


class Flow:
    def __init__(self, term):
        self.steps = reduction(term)
        self.flying = next(self.steps)
        self.result = None

    def advance(self, arrived):
        try:
            self.flying = self.steps.send(arrived)
        except StopIteration as stop:
            self.flying, self.result = [], stop.value


def fence(values, *flows):
    flows = [flow for flow in flows if flow.result is None]
    values, arrived = lax.optimization_barrier((values, [flow.flying for flow in flows]))
    for flow, came in zip(flows, arrived):
        flow.advance(came)
    return values


def drained(*flows):
    while any(flow.result is None for flow in flows):
        for flow in flows:
            if flow.result is None:
                flow.advance(flow.flying)
    return [flow.result for flow in flows]


def summed_everywhere(term):
    for axis in ("dp", "space"):
        for bit in range(bits_of(axis)):
            term = term + swap(term, axis, bit)
    return term


def shards(
    mixed_two,
    input_two,
    cotangent,
    w_in_two,
    w_out_two,
    kernel_two,
    mixed_one,
    w_in_one,
    w_out_one,
    kernel_one,
):
    shape4 = mixed_two.shape
    channels = shape4[3]
    inv_batch = 1.0 / (shape4[0] * lax.axis_size("dp"))
    mixed_flat = mixed_two.reshape(-1, channels)
    cot_flat = cotangent.reshape(-1, channels)
    preact = lax.dot_general(
        mixed_flat, w_in_two, CONTRACT_LAST, preferred_element_type=jnp.float32
    )
    activation, gelu_slope = gelu_parts(preact)
    activation = activation.astype(jnp.bfloat16)

    out_term = (
        lax.dot_general(activation, cot_flat, CONTRACT_FIRST, preferred_element_type=jnp.float32)
        * inv_batch
    ).astype(jnp.bfloat16)
    cot_late, out_term = fence((cot_flat, out_term))
    out_flow = Flow(out_term)
    hidden_grad = lax.dot_general(
        cot_late, w_out_two, CONTRACT_LAST, preferred_element_type=jnp.float32
    )
    pre_grad = (hidden_grad * gelu_slope).astype(jnp.bfloat16)
    in_term = (
        lax.dot_general(pre_grad, mixed_flat, CONTRACT_FIRST, preferred_element_type=jnp.float32)
        * inv_batch
    ).astype(jnp.bfloat16)
    pre_grad, in_term = fence((pre_grad, in_term), out_flow)
    in_flow = Flow(in_term)
    mix_grad = (
        jnp.dot(pre_grad, w_in_two, preferred_element_type=jnp.float32)
        .astype(jnp.bfloat16)
        .reshape(shape4)
    )
    in_before, in_after = edge_rows(input_two)
    mix_grad, mixed_one = fence((mix_grad, mixed_one), out_flow, in_flow)
    edges = edge_rows(mix_grad)
    preact_early = lax.dot_general(
        mixed_one.reshape(-1, channels), w_in_one, CONTRACT_LAST, preferred_element_type=jnp.float32
    )
    grad_two, taps_term = conv_call(
        late_kernel,
        cotangent,
        kernel_two,
        edges,
        mix_grad,
        [in_before, input_two, in_after],
        True,
    )
    grad_two, preact_early = fence((grad_two, preact_early), out_flow, in_flow)
    unused_act, slope_early = gelu_parts(preact_early)
    hidden_early = lax.dot_general(
        grad_two.reshape(-1, channels), w_out_one, CONTRACT_LAST, preferred_element_type=jnp.float32
    )
    pre_early = (hidden_early * slope_early).astype(jnp.bfloat16)
    mix_early = (
        jnp.dot(pre_early, w_in_one, preferred_element_type=jnp.float32)
        .astype(jnp.bfloat16)
        .reshape(shape4)
    )
    mix_early = fence(mix_early, out_flow, in_flow)
    (grad_one,) = conv_call(
        early_kernel, grad_two, kernel_one, edge_rows(mix_early), mix_early, [], False
    )
    grad_one, taps_term = fence((grad_one, taps_term), out_flow, in_flow)
    grad_kernel = summed_everywhere(jnp.sum(taps_term, axis=0) * inv_batch)
    grad_w_out, grad_w_in = drained(out_flow, in_flow)
    return (grad_one, grad_w_in, grad_w_out, grad_kernel)


def solution(mesh):
    return jax.shard_map(
        shards,
        mesh=mesh,
        in_specs=(
            P("dp", "space", None, None),
            P("dp", "space", None, None),
            P("dp", "space", None, None),
            P(),
            P(),
            P(),
            P("dp", "space", None, None),
            P(),
            P(),
            P(),
        ),
        out_specs=(P("dp", "space", None, None), P("dp", None), P("dp", None), P()),
        check_vma=False,
    )
```

```python
import math

import jax
import jax.numpy as jnp
from jax import lax
from jax.experimental import pallas as pl
from jax.experimental.pallas import tpu as pltpu
from jax.sharding import PartitionSpec as P

GELU_C = math.sqrt(2.0 / math.pi)
CONTRACT_LAST = (((1,), (1,)), ((), ()))
CONTRACT_FIRST = (((0,), (0,)), ((), ()))


LANES = 128


def edge_rows(fields):
    count = lax.axis_size("space")
    ends = count - 1
    head = jnp.concatenate([cells[:, :1] for cells in fields], axis=1)
    tail = jnp.concatenate([cells[:, -1:] for cells in fields], axis=1)
    before = lax.ppermute(tail, "space", [(i, i + 1) for i in range(ends)])
    after = lax.ppermute(head, "space", [(i + 1, i) for i in range(ends)])
    return before, after


def rolled(row, shift):
    if shift == 0:
        return row
    if shift == 1:
        return jnp.concatenate([row[-1:], row[:-1]], axis=0)
    return jnp.concatenate([row[1:], row[:1]], axis=0)


def spread(ref_before, ref, ref_after, index, band_rows):
    if index == 0:
        return ref_before[0, 0]
    if index == band_rows + 1:
        return ref_after[0, 0]
    return ref[0, index - 1]


def conv_accumulate(out_ref, base_ref, kernel_ref, before_ref, grad_ref, after_ref, visit):
    band_rows = grad_ref.shape[1]
    taps = kernel_ref[...].astype(jnp.float32)
    windows = {}
    for i in range(band_rows):
        for p in range(i, i + 3):
            if p not in windows:
                row = spread(before_ref, grad_ref, after_ref, p, band_rows).astype(jnp.float32)
                windows[p] = [rolled(row, b - 1) for b in range(3)]
        total = base_ref[0, i].astype(jnp.float32)
        for lat in range(3):
            for lon in range(3):
                tap = 3 * lat + lon
                total = total + taps[tap : tap + 1] * windows[i + 2 - lat][lon]
        out_ref[0, i] = total.astype(out_ref.dtype)
        visit(i, windows[i + 1])
        del windows[i]


def late_kernel(
    base_ref, kernel_ref, before_ref, grad_ref, after_ref,
    in_before_ref, in_ref, in_after_ref, out_ref, taps_ref,
):
    band_rows = grad_ref.shape[1]
    taps_ref[...] = jnp.zeros_like(taps_ref)

    def visit(i, shifted):
        for lat in range(3):
            row = spread(in_before_ref, in_ref, in_after_ref, i + lat, band_rows)
            row = row.astype(jnp.float32)
            for lon in range(3):
                tap = 3 * lat + lon
                taps_ref[tap : tap + 1, :] += jnp.sum(row * shifted[lon], axis=0, keepdims=True)

    conv_accumulate(out_ref, base_ref, kernel_ref, before_ref, grad_ref, after_ref, visit)


def early_kernel(base_ref, kernel_ref, before_ref, grad_ref, after_ref, out_ref):
    conv_accumulate(
        out_ref, base_ref, kernel_ref, before_ref, grad_ref, after_ref, lambda i, w: None
    )


def conv_call(kernel_fn, base, kernel, edges, grad, stored):
    samples, rows, columns, channels = grad.shape
    taps = kernel.shape[0]

    with_taps = stored is not None

    def field(count, first=0):
        return pl.BlockSpec((1, count, columns, LANES), lambda s, c: (s, first, 0, c))

    tap_spec = pl.BlockSpec((taps, LANES), lambda s, c: (0, c))
    in_specs = [field(rows), tap_spec, field(1), field(rows), field(1)]
    args = [base, kernel, edges[0], grad, edges[1]]
    out_shape = [jax.ShapeDtypeStruct(grad.shape, jnp.bfloat16)]
    out_specs = [field(rows)]
    if with_taps:
        in_specs += [field(1, 1), field(rows), field(1, 1)]
        args += [edges[0], stored, edges[1]]
        out_shape.append(jax.ShapeDtypeStruct((samples, taps, channels), jnp.float32))
        out_specs.append(pl.BlockSpec((None, taps, LANES), lambda s, c: (s, 0, c)))
    work = grad.size * (40 if with_taps else 20)
    return pl.pallas_call(
        kernel_fn,
        grid=(samples, channels // LANES),
        in_specs=in_specs,
        out_specs=out_specs,
        out_shape=out_shape,
        compiler_params=pltpu.CompilerParams(
            dimension_semantics=("arbitrary", "arbitrary"), vmem_limit_bytes=24 * 1024 * 1024
        ),
        cost_estimate=pl.CostEstimate(
            flops=work, bytes_accessed=grad.size * 8, transcendentals=0
        ),
    )(*args)


def gelu_parts(preact):
    tanh_arg = GELU_C * (preact + 0.044715 * preact * preact * preact)
    tanh_val = jnp.tanh(tanh_arg)
    activation = 0.5 * preact * (1.0 + tanh_val)
    gelu_slope = 0.5 * (1.0 + tanh_val) + 0.5 * preact * (1.0 - tanh_val * tanh_val) * GELU_C * (
        1.0 + 3.0 * 0.044715 * preact * preact
    )
    return (activation, gelu_slope)


def bits_of(axis):
    return (lax.axis_size(axis) - 1).bit_length()


def swap(cells, axis, bit):
    count = lax.axis_size(axis)
    return lax.ppermute(cells, axis, [(i, i ^ (1 << bit)) for i in range(count)])


def my_bit(axis, bit):
    return (lax.axis_index(axis) // (1 << bit)) % 2


def split(cells, labels, axis, bit):
    dim = labels.index((axis, bit))
    mine = my_bit(axis, bit)
    sent = lax.dynamic_index_in_dim(cells, 1 - mine, dim, keepdims=False)
    kept = lax.dynamic_index_in_dim(cells, mine, dim, keepdims=False)
    return kept, swap(sent, axis, bit), labels[:dim] + labels[dim + 1 :]


def merged(kept, came):
    return (kept.astype(jnp.float32) + came.astype(jnp.float32)).astype(jnp.bfloat16)


def reduction(term):
    dp_bits, space_bits = bits_of("dp"), bits_of("space")
    labels = [("dp", bit) for bit in reversed(range(dp_bits))]
    labels += [("space", bit) for bit in reversed(range(space_bits))]
    width = term.shape[1]
    cells = term.reshape((2,) * len(labels) + (-1, width))
    kept, came, labels = split(cells, labels, "dp", 0)
    (came,) = yield [came]
    cells = merged(kept, came)
    halves = [
        lax.slice_in_dim(cells, part * width // 2, (part + 1) * width // 2, axis=cells.ndim - 1)
        for part in range(2)
    ]
    space_order = list(range(space_bits))
    left = [labels, labels]
    for step in range(space_bits):
        bits = (space_order[step], space_order[-1 - step])
        moved = [split(halves[p], left[p], "space", bits[p]) for p in range(2)]
        left = [m[2] for m in moved]
        arrived = yield [m[1] for m in moved]
        halves = [merged(m[0], c) for m, c in zip(moved, arrived)]
    rows, labels = jnp.concatenate(halves, axis=-1), left[0]
    for bit in range(1, dp_bits):
        kept, came, labels = split(rows, labels, "dp", bit)
        (came,) = yield [came]
        rows = merged(kept, came)
    rows = rows[None]
    for bit in range(space_bits):
        (other,) = yield [swap(rows, "space", bit)]
        low = my_bit("space", bit) == 0
        rows = jnp.concatenate(
            [jnp.where(low, rows, other), jnp.where(low, other, rows)], axis=0
        )
    return rows.reshape(-1, width).astype(jnp.float32)


class Flow:
    def __init__(self, steps):
        self.steps = steps
        self.flying = next(self.steps)
        self.result = None

    def advance(self, arrived):
        try:
            self.flying = self.steps.send(arrived)
        except StopIteration as stop:
            self.flying, self.result = [], stop.value


def fence(values, *flows):
    flows = [flow for flow in flows if flow.result is None]
    values, arrived = lax.optimization_barrier((values, [flow.flying for flow in flows]))
    for flow, came in zip(flows, arrived):
        flow.advance(came)
    return values


def drained(*flows):
    while any(flow.result is None for flow in flows):
        for flow in flows:
            if flow.result is None:
                flow.advance(flow.flying)
    return [flow.result for flow in flows]


def summed_everywhere(term):
    for axis in ("dp", "space"):
        for bit in range(bits_of(axis)):
            (other,) = yield [swap(term, axis, bit)]
            term = term + other
    return term


def shards(
    mixed_two,
    input_two,
    cotangent,
    w_in_two,
    w_out_two,
    kernel_two,
    mixed_one,
    w_in_one,
    w_out_one,
    kernel_one,
):
    shape4 = mixed_two.shape
    channels = shape4[3]
    inv_batch = 1.0 / (shape4[0] * lax.axis_size("dp"))
    mixed_flat = mixed_two.reshape(-1, channels)
    cot_flat = cotangent.reshape(-1, channels)
    preact = lax.dot_general(
        mixed_flat, w_in_two, CONTRACT_LAST, preferred_element_type=jnp.float32
    )
    activation, gelu_slope = gelu_parts(preact)
    activation = activation.astype(jnp.bfloat16)

    out_term = (
        lax.dot_general(activation, cot_flat, CONTRACT_FIRST, preferred_element_type=jnp.float32)
        * inv_batch
    ).astype(jnp.bfloat16)
    cot_late, out_term = fence((cot_flat, out_term))
    out_flow = Flow(reduction(out_term))
    hidden_grad = lax.dot_general(
        cot_late, w_out_two, CONTRACT_LAST, preferred_element_type=jnp.float32
    )
    pre_grad = (hidden_grad * gelu_slope).astype(jnp.bfloat16)
    in_term = (
        lax.dot_general(pre_grad, mixed_flat, CONTRACT_FIRST, preferred_element_type=jnp.float32)
        * inv_batch
    ).astype(jnp.bfloat16)
    pre_grad, in_term = fence((pre_grad, in_term), out_flow)
    in_flow = Flow(reduction(in_term))
    mix_grad = (
        jnp.dot(pre_grad, w_in_two, preferred_element_type=jnp.float32)
        .astype(jnp.bfloat16)
        .reshape(shape4)
    )
    before, after = edge_rows([mix_grad, input_two])
    preact_early = lax.dot_general(
        mixed_one.reshape(-1, channels), w_in_one, CONTRACT_LAST, preferred_element_type=jnp.float32
    )
    mix_grad, before, after, preact_early = fence(
        (mix_grad, before, after, preact_early), out_flow, in_flow
    )
    grad_two, taps_term = conv_call(
        late_kernel, cotangent, kernel_two, (before, after), mix_grad, input_two
    )
    grad_two, preact_early, taps_term = fence(
        (grad_two, preact_early, taps_term), out_flow, in_flow
    )
    taps_flow = Flow(summed_everywhere(jnp.sum(taps_term, axis=0) * inv_batch))
    unused_act, slope_early = gelu_parts(preact_early)
    hidden_early = lax.dot_general(
        grad_two.reshape(-1, channels), w_out_one, CONTRACT_LAST, preferred_element_type=jnp.float32
    )
    pre_early = (hidden_early * slope_early).astype(jnp.bfloat16)
    mix_early = (
        jnp.dot(pre_early, w_in_one, preferred_element_type=jnp.float32)
        .astype(jnp.bfloat16)
        .reshape(shape4)
    )
    mix_early = fence(mix_early, out_flow, in_flow, taps_flow)
    (grad_one,) = conv_call(
        early_kernel, grad_two, kernel_one, edge_rows([mix_early]), mix_early, None
    )
    grad_one = fence(grad_one, out_flow, in_flow, taps_flow)
    grad_w_out, grad_w_in, grad_kernel = drained(out_flow, in_flow, taps_flow)
    return (grad_one, grad_w_in, grad_w_out, grad_kernel)


def solution(mesh):
    return jax.shard_map(
        shards,
        mesh=mesh,
        in_specs=(
            P("dp", "space", None, None),
            P("dp", "space", None, None),
            P("dp", "space", None, None),
            P(),
            P(),
            P(),
            P("dp", "space", None, None),
            P(),
            P(),
            P(),
        ),
        out_specs=(P("dp", "space", None, None), P("dp", None), P("dp", None), P()),
        check_vma=False,
    )
```
